16 devices in a mesh: rep: 1, dp: 16 (over x, y, z, core).
Axes of the slice: x: 2, y: 2, z: 2, core: 2. Of those that a mesh axis runs over, the one named last changes fastest.
Arguments:
- a: bfloat16 [16, 4, 4096, 1024], P(('rep', 'dp'))
- g: bfloat16 [16, 4, 4096, 3328], P(('rep', 'dp'))
Outputs:
- output: bfloat16 [4, 1024, 3328], P('rep')
All inputs are finite; a program needn't handle non-finite values.
Results may differ from the reference program's by a relative error of at most 0.012.
Values are sent between devices in bfloat16 or wider.
A program may use at most 2 GiB of HBM per device.

```python
import jax
import jax.numpy as jnp
from jax import lax

DEVICES = 16
MATRICES = 4
TOKENS = 4096
D = 1024
FF = 3328


def setup_inputs(seed: int = 0, part: int = 0) -> dict:
    ka, kg, ks = (jax.random.fold_in(k, part) for k in jax.random.split(jax.random.key(seed), 3))
    size = 2.0 ** jax.random.uniform(ks, (DEVICES, MATRICES, 1, 1), jnp.float32, -1.0, 1.0)
    a = jax.random.normal(ka, (DEVICES, MATRICES, TOKENS, D), jnp.float32)
    g = size * jax.random.normal(kg, (DEVICES, MATRICES, TOKENS, FF), jnp.float32) * (DEVICES * TOKENS) ** -0.5
    return {"a": a.astype(jnp.bfloat16), "g": g.astype(jnp.bfloat16)}


def reference(a, g):
    def take(so_far, one):
        return so_far + jnp.einsum("ntd,ntf->ndf", *one, preferred_element_type=jnp.float32), None

    return lax.scan(take, jnp.zeros((MATRICES, D, FF), jnp.float32), (a, g))[0].astype(jnp.bfloat16)
```

```python
import functools

import jax
import jax.numpy as jnp
from jax import lax
from jax.experimental import pallas as pl
from jax.experimental.pallas import tpu as pltpu
from jax.sharding import PartitionSpec as P

MESH = pl.DeviceIdType.MESH
W = 256
KC = 256
STAGE = 8
RS0, RS1, RS2, AG0, AG1, AG2, AG3, END = 2, 5, 7, 9, 11, 16, 19, 21
S_GO, S_GOT, S_RS, S_AG = 3, 4, 6, 12


def kernel(
    a, g, out, aT, stage, gbuf, full, own, core_s, core_r, k1, s1, r1, k2, s2, r2, k3, s3, r3,
    a_sem, g_sem, o_sem, send_c, recv_c, send_rs, recv_rs, send_ag, recv_ag,
):
    _, n_mat, depth, rows = a.shape
    tiles = g.shape[-1] // W
    units, chunks = n_mat * tiles, depth // KC
    half = rows // 2
    f32, bf16 = jnp.float32, jnp.bfloat16

    me = lax.axis_index("dp")
    core, z, y, x = me % 2, (me // 2) % 2, (me // 4) % 2, me // 8
    other = me + 1 - 2 * core
    near = (me + 8 - 16 * x, me + 4 - 8 * y, me + 2 - 4 * z)

    barrier = pltpu.get_barrier_semaphore()
    for d in (other, *near):
        pl.semaphore_signal(barrier, inc=1, device_id={"dp": d}, device_id_type=MESH)

    def pick(k, options):
        return jnp.where(k == 0, options[0], jnp.where(k == 1, options[1], options[2]))

    def axis(u, turn):
        k = (u + 2 * turn) % 3
        return pick(k, near), pick(k, (x, y, z))

    def spot(u, level):
        base, size = core * half, half
        for turn in range(level):
            size //= 2
            base = base + axis(u, turn)[1] * size
        base = pl.multiple_of(base, size)
        column = pl.multiple_of((u % tiles) * W, W)
        return full.at[u // tiles, pl.ds(base, size), pl.ds(column, W)]

    def remote(src, dst, send, recv, to):
        return pltpu.make_async_remote_copy(
            src_ref=src, dst_ref=dst, send_sem=send, recv_sem=recv, device_id={"dp": to}, device_id_type=MESH
        )

    def swap(u):
        return remote(core_s.at[u % S_GO], core_r.at[u % S_GOT], send_c.at[u % S_GO], recv_c.at[u % S_GOT], other)

    def scatter(u, turn):
        i = u % S_RS
        src, dst = ((s1, r1), (s2, r2), (s3, r3))[turn]
        return remote(src.at[i], dst.at[i], send_rs.at[turn, i], recv_rs.at[turn, i], axis(u, turn)[0])

    def gather(u, turn):
        i = u % S_AG
        place = spot(u, 3 - turn)
        to = other if turn == 3 else axis(u, 2 - turn)[0]
        return remote(place, place, send_ag.at[turn, i], recv_ag.at[turn, i], to)

    def store_out(u):
        column = pl.multiple_of((u % tiles) * W, W)
        at = (u // tiles, slice(None), pl.ds(column, W))
        return pltpu.make_async_copy(full.at[at], out.at[at], o_sem.at[u % 2])

    def load_g(u):
        column = pl.multiple_of((u % tiles) * W, W)
        return pltpu.make_async_copy(g.at[0, u // tiles, :, pl.ds(column, W)], gbuf.at[u % 3], g_sem.at[u % 3])

    def load_a(n, q):
        row = pl.multiple_of(q * KC, KC)
        return pltpu.make_async_copy(a.at[0, n, pl.ds(row, KC), :], stage.at[q % STAGE], a_sem.at[q % STAGE])

    def turn_a(n, q):
        load_a(n, q).wait()
        aT[n % 2, :, pl.ds(pl.multiple_of(q * KC, KC), KC)] = stage[q % STAGE].T

    def halve(u, turn, mine, came, keep, send):
        size = came.shape[0] // 2
        bit = axis(u, turn)[1]
        theirs = pl.ds(pl.multiple_of((1 - bit) * size, size), size)
        ours = pl.ds(pl.multiple_of(bit * size, size), size)
        send[...] = (mine[theirs, :] + came[theirs, :].astype(f32)).astype(bf16)
        scatter(u, turn).start()
        keep[...] = mine[ours, :] + came[ours, :].astype(f32)

    def rs0(u):
        swap(u).wait_recv()
        halve(u, 0, own, core_r.at[u % S_GOT], k1.at[u % 3], s1.at[u % S_RS])

    def rs1(u):
        scatter(u, 0).wait_recv()
        halve(u, 1, k1.at[u % 3], r1.at[u % S_RS], k2.at[u % 3], s2.at[u % S_RS])
        swap(u).wait_send()

    def rs2(u):
        scatter(u, 1).wait_recv()
        halve(u, 2, k2.at[u % 3], r2.at[u % S_RS], k3.at[u % 3], s3.at[u % S_RS])

    def ag0(u):
        scatter(u, 2).wait_recv()
        spot(u, 3)[...] = (k3[u % 3] + r3[u % S_RS].astype(f32)).astype(bf16)
        gather(u, 0).start()
        scatter(u, 0).wait_send()

    def ag1(u):
        gather(u, 0).wait_recv()
        gather(u, 1).start()
        scatter(u, 1).wait_send()

    def ag2(u):
        gather(u, 1).wait_recv()
        gather(u, 2).start()
        scatter(u, 2).wait_send()
        gather(u, 0).wait_send()

    def ag3(u):
        gather(u, 2).wait_recv()
        gather(u, 3).start()
        gather(u, 1).wait_send()

    def end(u):
        gather(u, 3).wait_recv()
        store_out(u).start()
        gather(u, 2).wait_send()
        gather(u, 3).wait_send()

    def end2(u):
        store_out(u).wait()

    phases = (
        (END + 2, end2), (END, end), (AG3, ag3), (AG2, ag2), (AG1, ag1), (AG0, ag0), (RS2, rs2), (RS1, rs1), (RS0, rs0)
    )

    ahead = min(STAGE, chunks)
    for q in range(ahead):
        load_a(0, q).start()
    load_g(0).start()
    load_g(1).start()

    def first(q, _):
        turn_a(0, q)

        @pl.when(q + ahead < chunks)
        def _():
            load_a(0, q + ahead).start()

    lax.fori_loop(0, chunks, first, None)
    pl.semaphore_wait(barrier, 4)

    def matmul(u, base):
        lhs = aT[(u // tiles) % 2, pl.ds(pl.multiple_of(base, half), half), :]
        return jnp.dot(lhs, gbuf[u % 3], preferred_element_type=f32)

    def step(t, _):
        for parity in range(2):
            for delay, phase in phases:
                if delay % 2 == parity:
                    u = t - delay // 2

                    @pl.when(jnp.logical_and(u >= 0, u < units))
                    def _(u=u, phase=phase):
                        phase(u)

            n, q = t // tiles + 1, 2 * (t % tiles) + parity

            @pl.when(jnp.logical_and(n < n_mat, q < chunks))
            def _():
                load_a(n, q).start()

            @pl.when(jnp.logical_and(n < n_mat, jnp.logical_and(q >= 2, q < chunks + 2)))
            def _():
                turn_a(n, q - 2)

            @pl.when(t < units)
            def _():
                if parity == 0:
                    load_g(t).wait()

                    @pl.when(t + 2 < units)
                    def _():
                        load_g(t + 2).start()

                    core_s[t % S_GO] = matmul(t, (1 - core) * half).astype(bf16)
                    swap(t).start()
                else:
                    own[...] = matmul(t, core * half)

    lax.fori_loop(0, units + END // 2 + 2, step, None)


def solution(mesh):
    def step(a, g):
        _, n_mat, depth, rows = a.shape
        columns = g.shape[-1]
        half = rows // 2
        f32, bf16 = jnp.float32, jnp.bfloat16
        q1, q2, q3 = half // 2, half // 4, half // 8
        DMA = pltpu.SemaphoreType.DMA
        return pl.pallas_call(
            kernel,
            name="grad_sums",
            out_shape=jax.ShapeDtypeStruct((n_mat, rows, columns), bf16),
            in_specs=[pl.BlockSpec(memory_space=pl.ANY)] * 2,
            out_specs=pl.BlockSpec(memory_space=pl.ANY),
            scratch_shapes=[
                pltpu.VMEM((2, rows, depth), bf16),
                pltpu.VMEM((STAGE, KC, rows), bf16),
                pltpu.VMEM((3, depth, W), bf16),
                pltpu.VMEM((n_mat, rows, columns), bf16),
                pltpu.VMEM((half, W), f32),
                pltpu.VMEM((S_GO, half, W), bf16),
                pltpu.VMEM((S_GOT, half, W), bf16),
                pltpu.VMEM((3, q1, W), f32),
                pltpu.VMEM((S_RS, q1, W), bf16),
                pltpu.VMEM((S_RS, q1, W), bf16),
                pltpu.VMEM((3, q2, W), f32),
                pltpu.VMEM((S_RS, q2, W), bf16),
                pltpu.VMEM((S_RS, q2, W), bf16),
                pltpu.VMEM((3, q3, W), f32),
                pltpu.VMEM((S_RS, q3, W), bf16),
                pltpu.VMEM((S_RS, q3, W), bf16),
                DMA((STAGE,)),
                DMA((3,)),
                DMA((2,)),
                DMA((S_GO,)),
                DMA((S_GOT,)),
                DMA((3, S_RS)),
                DMA((3, S_RS)),
                DMA((4, S_AG)),
                DMA((4, S_AG)),
            ],
            compiler_params=pltpu.CompilerParams(
                collective_id=0, has_side_effects=True, vmem_limit_bytes=67043328
            ),
            cost_estimate=pl.CostEstimate(
                flops=2 * n_mat * depth * rows * columns, bytes_accessed=2 * n_mat * (depth * (rows + columns)), transcendentals=0
            ),
        )(a, g)

    return jax.shard_map(
        step,
        mesh=mesh,
        in_specs=(P(("rep", "dp")), P(("rep", "dp"))),
        out_specs=P("rep"),
        check_vma=False,
    )
```

```python
import functools

import jax
import jax.numpy as jnp
from jax import lax
from jax.experimental import pallas as pl
from jax.experimental.pallas import tpu as pltpu
from jax.sharding import PartitionSpec as P

MESH = pl.DeviceIdType.MESH


def rem(x, n):
    return lax.rem(jnp.int32(x), jnp.int32(n))


def div(x, n):
    return lax.div(jnp.int32(x), jnp.int32(n))


class Unit:
    def __init__(self, three, plus):
        self.third = plus % 3
        self.three = three + plus // 3
        self.at = 3 * three + plus


W = 256
KC = 256
STAGE = 4
RS0, RS1, RS2, AG0, AG1, AG2, AG3, END = 2, 6, 9, 13, 19, 24, 33, 40
SPIN = 1
S_GO, S_GOT, S_RS, S_AG, S_END, K1, K2, K3 = 3, 6, 9, 18, 21, 3, 3, 3


def kernel(
    a, g, full, aT, stage, gbuf, own, core_s, core_r, k1, s1, r1, k2, s2, r2, k3, s3, r3,
    a_sem, g_sem, send_c, recv_c, send_rs, recv_rs, send_ag, recv_ag,
    send_end, recv_end,
):
    _, n_mat, depth, rows = a.shape
    tiles = g.shape[-1] // W
    units, chunks = n_mat * tiles, depth // KC
    half = rows // 2
    f32, bf16 = jnp.float32, jnp.bfloat16

    me = lax.axis_index("dp")
    core, z, y, x = rem(me, 2), rem(div(me, 2), 2), rem(div(me, 4), 2), div(me, 8)
    other = me + 1 - 2 * core
    near = (me + 8 - 16 * x, me + 4 - 8 * y, me + 2 - 4 * z)

    barrier = pltpu.get_barrier_semaphore()
    for d in (other, *near):
        pl.semaphore_signal(barrier, inc=1, device_id={"dp": d}, device_id_type=MESH)

    def axis(u, turn):
        k = (u.third + SPIN * turn) % 3
        return near[k], (x, y, z)[k]

    def slot(u, n):
        return u.third if n == 3 else 3 * rem(u.three, n // 3) + u.third

    def bounds(u, level):
        base, size = core * half, half
        for turn in range(level):
            size //= 2
            base = base + axis(u, turn)[1] * size
        return base, size

    def rows_of(u, base, size):
        column = pl.multiple_of(rem(u.at, tiles) * W, W)
        return full.at[div(u.at, tiles), pl.ds(pl.multiple_of(base, size), size), pl.ds(column, W)]

    def remote(src, dst, send, recv, to):
        return pltpu.make_async_remote_copy(
            src_ref=src, dst_ref=dst, send_sem=send, recv_sem=recv, device_id={"dp": to}, device_id_type=MESH
        )

    def swap(u):
        return remote(core_s.at[slot(u, S_GO)], core_r.at[slot(u, S_GOT)], send_c.at[slot(u, S_GO)], recv_c.at[slot(u, S_GOT)], other)

    def scatter(u, turn):
        i = slot(u, S_RS)
        src, dst = ((s1, r1), (s2, r2), (s3, r3))[turn]
        return remote(src.at[i], dst.at[i], send_rs.at[turn, i], recv_rs.at[turn, i], axis(u, turn)[0])

    def gather(u, kind):
        if kind == 6:
            i = slot(u, S_END)
            place = rows_of(u, core * half, half)
            return remote(place, place, send_end.at[i], recv_end.at[i], other)
        i = slot(u, S_AG)
        turn = (2, 1, 0, 1, 0, 0)[kind]
        base, size = bounds(u, 3)
        if kind in (3, 4):
            base = base + (1 - 2 * axis(u, 2)[1]) * size
        if kind == 5:
            base, size = bounds(u, 2)
            base = base + (1 - 2 * axis(u, 1)[1]) * size
        place = rows_of(u, base, size)
        return remote(place, place, send_ag.at[kind, i], recv_ag.at[kind, i], axis(u, turn)[0])

    def load_g(u):
        column = pl.multiple_of((rem(u.at, tiles)) * W, W)
        return pltpu.make_async_copy(g.at[0, div(u.at, tiles), :, pl.ds(column, W)], gbuf.at[slot(u, 3)], g_sem.at[slot(u, 3)])

    def load_a(n, q):
        row = pl.multiple_of(q * KC, KC)
        return pltpu.make_async_copy(a.at[0, n, pl.ds(row, KC), :], stage.at[rem(q, STAGE)], a_sem.at[rem(q, STAGE)])

    def turn_a(n, q):
        load_a(n, q).wait()
        aT[rem(n, 2), :, pl.ds(pl.multiple_of(q * KC, KC), KC)] = stage[rem(q, STAGE)].T

    def halve(u, turn, mine, came, keep, send):
        size = came.shape[0] // 2
        bit = axis(u, turn)[1]
        theirs = pl.ds(pl.multiple_of((1 - bit) * size, size), size)
        ours = pl.ds(pl.multiple_of(bit * size, size), size)
        send[...] = (mine[theirs, :] + came[theirs, :].astype(f32)).astype(bf16)
        scatter(u, turn).start()
        keep[...] = mine[ours, :] + came[ours, :].astype(f32)

    def rs0(u):
        swap(u).wait_recv()
        swap(u).wait_send()
        halve(u, 0, own, core_r.at[slot(u, S_GOT)], k1.at[slot(u, K1)], s1.at[slot(u, S_RS)])

    def rs1(u):
        scatter(u, 0).wait_recv()
        halve(u, 1, k1.at[slot(u, K1)], r1.at[slot(u, S_RS)], k2.at[slot(u, K2)], s2.at[slot(u, S_RS)])

    def rs2(u):
        scatter(u, 1).wait_recv()
        halve(u, 2, k2.at[slot(u, K2)], r2.at[slot(u, S_RS)], k3.at[slot(u, K3)], s3.at[slot(u, S_RS)])

    def ag0(u):
        scatter(u, 2).wait_recv()
        rows_of(u, *bounds(u, 3))[...] = (k3[slot(u, K3)] + r3[slot(u, S_RS)].astype(f32)).astype(bf16)
        for kind in (0, 1, 2):
            gather(u, kind).start()
        scatter(u, 0).wait_send()

    def ag1(u):
        gather(u, 0).wait_recv()
        gather(u, 3).start()
        gather(u, 4).start()
        scatter(u, 1).wait_send()

    def ag2(u):
        gather(u, 1).wait_recv()
        gather(u, 3).wait_recv()
        gather(u, 5).start()
        scatter(u, 2).wait_send()

    def ag3(u):
        for kind in (2, 4, 5):
            gather(u, kind).wait_recv()
        gather(u, 6).start()

    def end(u):
        gather(u, 6).wait_recv()
        for kind in range(7):
            gather(u, kind).wait_send()

    phases = (
        (END, end), (AG3, ag3), (AG2, ag2), (AG1, ag1), (AG0, ag0), (RS2, rs2), (RS1, rs1), (RS0, rs0)
    )

    side = rows // KC

    def raw(q):
        return pl.ds(pl.multiple_of((rem(q, side)) * KC, KC), KC), pl.ds(pl.multiple_of((div(q, side)) * rows, rows), rows)

    def load_first(q):
        row = pl.multiple_of(q * KC, KC)
        at = raw(q)
        return pltpu.make_async_copy(a.at[0, 0, pl.ds(row, KC), :], aT.at[1, at[0], at[1]], a_sem.at[q])

    for q in range(chunks):
        load_first(q).start()
    load_g(Unit(0, 0)).start()
    load_g(Unit(0, 1)).start()

    def first(q, _):
        load_first(q).wait()
        at = raw(q)
        aT[0, :, pl.ds(pl.multiple_of(q * KC, KC), KC)] = aT[1, at[0], at[1]].T

    lax.fori_loop(0, chunks, first, None)
    pl.semaphore_wait(barrier, 4)

    def matmul(u, base):
        lhs = aT[rem(div(u.at, tiles), 2), pl.ds(pl.multiple_of(base, half), half), :]
        return jnp.dot(lhs, gbuf[slot(u, 3)], preferred_element_type=f32)

    def three(i, _):
        for plus in range(3):
            for parity in range(2):
                half_step(i, plus, parity)

    def half_step(i, plus, parity):
        unit = Unit(i, plus)
        t = unit.at
        for delay, phase in phases:
            if delay % 2 == parity:
                u = Unit(i, plus - delay // 2)

                @pl.when(jnp.logical_and(u.at >= 0, u.at < units))
                def _(u=u, phase=phase):
                    phase(u)

        n, q = div(t, tiles) + 1, 2 * rem(t, tiles) + parity - (2 * tiles - chunks - 2)

        @pl.when(jnp.logical_and(n < n_mat, jnp.logical_and(q >= 0, q < chunks)))
        def _():
            load_a(n, q).start()

        @pl.when(jnp.logical_and(n < n_mat, jnp.logical_and(q >= 2, q < chunks + 2)))
        def _():
            turn_a(n, q - 2)

        @pl.when(t < units)
        def _():
            if parity == 0:
                load_g(unit).wait()

                @pl.when(t + 2 < units)
                def _():
                    load_g(Unit(i, plus + 2)).start()

                core_s[slot(unit, S_GO)] = matmul(unit, (1 - core) * half).astype(bf16)
                swap(unit).start()
            else:
                own[...] = matmul(unit, core * half)

    lax.fori_loop(0, (units + END // 2 + 2) // 3 + 1, three, None)


def solution(mesh):
    def step(a, g):
        _, n_mat, depth, rows = a.shape
        columns = g.shape[-1]
        half = rows // 2
        f32, bf16 = jnp.float32, jnp.bfloat16
        q1, q2, q3 = half // 2, half // 4, half // 8
        DMA = pltpu.SemaphoreType.DMA
        sums = pl.pallas_call(
            kernel,
            name="grad_sums",
            out_shape=pltpu.VMEM((n_mat, rows, columns), bf16),
            in_specs=[pl.BlockSpec(memory_space=pl.ANY)] * 2,
            out_specs=pl.BlockSpec(memory_space=pltpu.VMEM),
            scratch_shapes=[
                pltpu.VMEM((2, rows, depth), bf16),
                pltpu.VMEM((STAGE, KC, rows), bf16),
                pltpu.VMEM((3, depth, W), bf16),
                pltpu.VMEM((half, W), f32),
                pltpu.VMEM((S_GO, half, W), bf16),
                pltpu.VMEM((S_GOT, half, W), bf16),
                pltpu.VMEM((K1, q1, W), f32),
                pltpu.VMEM((S_RS, q1, W), bf16),
                pltpu.VMEM((S_RS, q1, W), bf16),
                pltpu.VMEM((K2, q2, W), f32),
                pltpu.VMEM((S_RS, q2, W), bf16),
                pltpu.VMEM((S_RS, q2, W), bf16),
                pltpu.VMEM((K3, q3, W), f32),
                pltpu.VMEM((S_RS, q3, W), bf16),
                pltpu.VMEM((S_RS, q3, W), bf16),
                DMA((depth // KC,)),
                DMA((3,)),
                DMA((S_GO,)),
                DMA((S_GOT,)),
                DMA((3, S_RS)),
                DMA((3, S_RS)),
                DMA((6, S_AG)),
                DMA((6, S_AG)),
                DMA((S_END,)),
                DMA((S_END,)),
            ],
            compiler_params=pltpu.CompilerParams(
                collective_id=0, has_side_effects=True, vmem_limit_bytes=34 * 2**20
            ),
            cost_estimate=pl.CostEstimate(
                flops=2 * n_mat * depth * rows * columns, bytes_accessed=2 * n_mat * (depth * (rows + columns)), transcendentals=0
            ),
        )(a, g)

        def place(src, dst, sem):
            copy = pltpu.make_async_copy(src, dst, sem)
            copy.start()
            copy.wait()

        return pl.pallas_call(
            place,
            name="place",
            out_shape=jax.ShapeDtypeStruct(sums.shape, sums.dtype),
            in_specs=[pl.BlockSpec(memory_space=pltpu.VMEM)],
            out_specs=pl.BlockSpec(memory_space=pl.ANY),
            scratch_shapes=[DMA],
            compiler_params=pltpu.CompilerParams(vmem_limit_bytes=2**20),
        )(sums)

    return jax.shard_map(
        step,
        mesh=mesh,
        in_specs=(P(("rep", "dp")), P(("rep", "dp"))),
        out_specs=P("rep"),
        check_vma=False,
    )
```
